16 devices in a mesh: dp: 4 (over z, y), tp: 4 (over x, core).
Axes of the slice: x: 2, y: 2, z: 2, core: 2. Of those that a mesh axis runs over, the one named last changes fastest.
Arguments:
- x_in: bfloat16 [4, 2048, 1536], P('dp', 'tp'), parts along dimension 0
- x_mid: bfloat16 [4, 2048, 1536], P('dp', 'tp'), parts along dimension 0
- d_out: bfloat16 [4, 2048, 1536], P('dp', 'tp'), parts along dimension 0
- q_saved: bfloat16 [4, 2048, 16, 96], P('dp', None, 'tp'), parts along dimension 0
- k_saved: bfloat16 [4, 2048, 16, 96], P('dp', None, 'tp'), parts along dimension 0
- v_saved: bfloat16 [4, 2048, 16, 96], P('dp', None, 'tp'), parts along dimension 0
- z_saved: bfloat16 [4, 2048, 6144], P('dp', None, 'tp'), parts along dimension 0
- ln1_gain: float32 [1536], replicated
- ln1_bias: float32 [1536], replicated
- ln2_gain: float32 [1536], replicated
- ln2_bias: float32 [1536], replicated
- w_qkv: bfloat16 [3, 1536, 16, 96], P(None, None, 'tp')
- w_proj: bfloat16 [16, 96, 1536], P('tp')
- w_fc1: bfloat16 [1536, 6144], P(None, 'tp')
- w_fc2: bfloat16 [6144, 1536], P('tp')
Outputs:
- output 1: bfloat16 [4, 2048, 1536], P('dp', 'tp'), parts along dimension 0
- output 2: float32 [12, 1536, 16, 96], P('dp', None, 'tp'), parts along dimension 0
- output 3: float32 [12, 16, 96], P('dp', 'tp'), parts along dimension 0
- output 4: float32 [64, 96, 1536], P(('dp', 'tp')), parts along dimension 0
- output 5: float32 [6144, 6144], P('dp', 'tp'), parts along dimension 0
- output 6: float32 [24576], P(('dp', 'tp')), parts along dimension 0
- output 7: float32 [24576, 1536], P(('dp', 'tp')), parts along dimension 0
- output 8: float32 [24, 1536], P('dp'), parts along dimension 0
There are 4 independent parts. The reference program is written for one: setup_inputs(seed, part) draws one part's arguments, and reference() takes and returns one part's arrays. A program takes and returns all parts, laid end to end along the dimension named above; an argument that names none is the same for every part.
All inputs are finite; a program needn't handle non-finite values.
Results may differ from the reference program's by a relative error of at most 0.0106856.
Values are sent between devices in bfloat16 or wider.
A program may use at most 1 GiB of HBM per device.

```python
import jax
import jax.numpy as jnp
from jax import lax

BATCH_SEQS = 1
SEQ_LEN = 2048
D_MODEL = 1536
N_HEADS = 16
HEAD_DIM = 96
FF_DIM = 6144
LN_EPS = 1e-5
GELU_COEF = 0.044715
GELU_SCALE = 0.7978845608028654


def draw_normal(key, shape, scale):
    return (scale * jax.random.normal(key, shape, jnp.float32)).astype(jnp.bfloat16)


def setup_inputs(seed: int = 0, part: int = 0) -> dict:
    part_keys = jax.random.split(jax.random.fold_in(jax.random.key(seed), part), 7)
    shared_keys = jax.random.split(jax.random.key(seed + 1), 8)
    tok_shape = (BATCH_SEQS, SEQ_LEN, D_MODEL)
    head_shape = (BATCH_SEQS, SEQ_LEN, N_HEADS, HEAD_DIM)
    return {
        'x_in': draw_normal(part_keys[0], tok_shape, 1.0),
        'x_mid': draw_normal(part_keys[1], tok_shape, 1.0),
        'd_out': draw_normal(part_keys[2], tok_shape, 1.0),
        'q_saved': draw_normal(part_keys[3], head_shape, 1.0),
        'k_saved': draw_normal(part_keys[4], head_shape, 1.0),
        'v_saved': draw_normal(part_keys[5], head_shape, 1.0),
        'z_saved': draw_normal(part_keys[6], (BATCH_SEQS, SEQ_LEN, FF_DIM), 1.5),
        'ln1_gain': jax.random.uniform(shared_keys[0], (D_MODEL,), jnp.float32, 0.5, 1.5),
        'ln1_bias': 0.5 * jax.random.normal(shared_keys[1], (D_MODEL,), jnp.float32),
        'ln2_gain': jax.random.uniform(shared_keys[2], (D_MODEL,), jnp.float32, 0.5, 1.5),
        'ln2_bias': 0.5 * jax.random.normal(shared_keys[3], (D_MODEL,), jnp.float32),
        'w_qkv': draw_normal(shared_keys[4], (3, D_MODEL, N_HEADS, HEAD_DIM), D_MODEL ** -0.5),
        'w_proj': draw_normal(shared_keys[5], (N_HEADS, HEAD_DIM, D_MODEL), D_MODEL ** -0.5),
        'w_fc1': draw_normal(shared_keys[6], (D_MODEL, FF_DIM), D_MODEL ** -0.5),
        'w_fc2': draw_normal(shared_keys[7], (FF_DIM, D_MODEL), FF_DIM ** -0.5),
    }


def layer_norm_fwd(token_rows, norm_gain, norm_bias):
    rows_f32 = token_rows.astype(jnp.float32)
    centered = rows_f32 - jnp.mean(rows_f32, axis=-1, keepdims=True)
    inv_std = lax.rsqrt(jnp.mean(centered * centered, axis=-1, keepdims=True) + LN_EPS)
    x_hat = centered * inv_std
    return x_hat, inv_std, (x_hat * norm_gain + norm_bias).astype(jnp.bfloat16)


def layer_norm_bwd(grad_norm, x_hat, inv_std, norm_gain):
    grad_hat = grad_norm * norm_gain
    centered_grad = grad_hat - jnp.mean(grad_hat, axis=-1, keepdims=True)
    return inv_std * (centered_grad - x_hat * jnp.mean(grad_hat * x_hat, axis=-1, keepdims=True))


def gelu_parts(pre_act):
    tanh_val = jnp.tanh(GELU_SCALE * (pre_act + GELU_COEF * pre_act * pre_act * pre_act))
    act_value = 0.5 * pre_act * (1.0 + tanh_val)
    act_slope = 0.5 * (1.0 + tanh_val) + 0.5 * pre_act * (1.0 - tanh_val * tanh_val) * GELU_SCALE * (1.0 + 3.0 * GELU_COEF * pre_act * pre_act)
    return act_value, act_slope


def head_attention_grads(operands):
    q_head, k_head, v_head, dctx_head = operands
    score_scale = HEAD_DIM ** -0.5
    q_wide = q_head.astype(jnp.float32)
    k_wide = k_head.astype(jnp.float32)
    v_wide = v_head.astype(jnp.float32)
    dctx_wide = dctx_head.astype(jnp.float32)
    scores = jnp.einsum('bqe,bke->bqk', q_wide, k_wide) * score_scale
    row_ids = lax.broadcasted_iota(jnp.int32, (SEQ_LEN, SEQ_LEN), 0)
    col_ids = lax.broadcasted_iota(jnp.int32, (SEQ_LEN, SEQ_LEN), 1)
    scores = jnp.where(row_ids >= col_ids, scores, -1e30)
    attn_probs = jax.nn.softmax(scores, axis=-1)
    probs_low = attn_probs.astype(jnp.bfloat16).astype(jnp.float32)
    context = jnp.einsum('bqk,bke->bqe', probs_low, v_wide).astype(jnp.bfloat16)
    grad_probs = jnp.einsum('bqe,bke->bqk', dctx_wide, v_wide)
    grad_scores = attn_probs * (grad_probs - jnp.sum(grad_probs * attn_probs, axis=-1, keepdims=True)) * score_scale
    scores_low = grad_scores.astype(jnp.bfloat16).astype(jnp.float32)
    grad_q = jnp.einsum('bqk,bke->bqe', scores_low, k_wide).astype(jnp.bfloat16)
    grad_k = jnp.einsum('bqk,bqe->bke', scores_low, q_wide).astype(jnp.bfloat16)
    grad_v = jnp.einsum('bqk,bqe->bke', probs_low, dctx_wide).astype(jnp.bfloat16)
    return context, grad_q, grad_k, grad_v


def reference(x_in, x_mid, d_out, q_saved, k_saved, v_saved, z_saved, ln1_gain, ln1_bias, ln2_gain, ln2_bias, w_qkv, w_proj, w_fc1, w_fc2):
    n_tok = BATCH_SEQS * SEQ_LEN
    norm2_hat, norm2_rstd, h2_norm = layer_norm_fwd(x_mid, ln2_gain, ln2_bias)
    act_value, act_slope = gelu_parts(z_saved.astype(jnp.float32))
    dout_rows = d_out.reshape(n_tok, D_MODEL)
    grad_wfc2 = jnp.dot(act_value.astype(jnp.bfloat16).reshape(n_tok, FF_DIM).T, dout_rows, preferred_element_type=jnp.float32)
    grad_act = jnp.dot(dout_rows, w_fc2.T, preferred_element_type=jnp.float32)
    grad_pre = (grad_act * act_slope.reshape(n_tok, FF_DIM)).astype(jnp.bfloat16)
    grad_wfc1 = jnp.dot(h2_norm.reshape(n_tok, D_MODEL).T, grad_pre, preferred_element_type=jnp.float32)
    grad_bfc1 = jnp.sum(grad_pre.astype(jnp.float32), axis=0)
    grad_h2 = jnp.dot(grad_pre, w_fc1.T, preferred_element_type=jnp.float32).reshape(BATCH_SEQS, SEQ_LEN, D_MODEL)
    grad_mid = (d_out.astype(jnp.float32) + layer_norm_bwd(grad_h2, norm2_hat, norm2_rstd, ln2_gain)).astype(jnp.bfloat16)
    mid_rows = grad_mid.reshape(n_tok, D_MODEL)
    grad_ctx = jnp.dot(mid_rows, w_proj.reshape(D_MODEL, D_MODEL).T, preferred_element_type=jnp.float32).astype(jnp.bfloat16)
    grad_ctx = grad_ctx.reshape(BATCH_SEQS, SEQ_LEN, N_HEADS, HEAD_DIM)
    context, grad_q, grad_k, grad_v = lax.map(head_attention_grads, (jnp.moveaxis(q_saved, 2, 0), jnp.moveaxis(k_saved, 2, 0), jnp.moveaxis(v_saved, 2, 0), jnp.moveaxis(grad_ctx, 2, 0)))
    context_rows = jnp.moveaxis(context, 0, 2).reshape(n_tok, D_MODEL)
    grad_wproj = jnp.dot(context_rows.T, mid_rows, preferred_element_type=jnp.float32).reshape(N_HEADS, HEAD_DIM, D_MODEL)
    norm1_hat, norm1_rstd, h1_norm = layer_norm_fwd(x_in, ln1_gain, ln1_bias)
    qkv_rows = jnp.moveaxis(jnp.stack([grad_q, grad_k, grad_v]), 1, 3).reshape(3, n_tok, D_MODEL).astype(jnp.float32)
    grad_wqkv = jnp.einsum('td,ite->ide', h1_norm.reshape(n_tok, D_MODEL).astype(jnp.float32), qkv_rows).reshape(3, D_MODEL, N_HEADS, HEAD_DIM)
    grad_bqkv = jnp.sum(qkv_rows, axis=1).reshape(3, N_HEADS, HEAD_DIM)
    grad_h1 = jnp.einsum('ite,ide->td', qkv_rows, w_qkv.reshape(3, D_MODEL, D_MODEL).astype(jnp.float32)).reshape(BATCH_SEQS, SEQ_LEN, D_MODEL)
    grad_x = (grad_mid.astype(jnp.float32) + layer_norm_bwd(grad_h1, norm1_hat, norm1_rstd, ln1_gain)).astype(jnp.bfloat16)
    grad_vecs = jnp.stack([
        jnp.sum(grad_h1 * norm1_hat, axis=(0, 1)),
        jnp.sum(grad_h1, axis=(0, 1)),
        jnp.sum(grad_h2 * norm2_hat, axis=(0, 1)),
        jnp.sum(grad_h2, axis=(0, 1)),
        jnp.sum(grad_mid.astype(jnp.float32), axis=(0, 1)),
        jnp.sum(d_out.astype(jnp.float32), axis=(0, 1)),
    ])
    return grad_x, grad_wqkv, grad_bqkv, grad_wproj, grad_wfc1, grad_bfc1, grad_wfc2, grad_vecs
```

```python
import functools

import jax
import jax.numpy as jnp
from jax import lax
from jax.experimental import pallas as pl
from jax.experimental.pallas import tpu as pltpu
from jax.sharding import PartitionSpec as P

LN_EPS = 1e-5
GELU_COEF = 0.044715
GELU_SCALE = 0.7978845608028654
LOG2E = 1.4426950408889634
NEG = -1e30
QB = 256


def layer_norm_fwd(token_rows, norm_gain, norm_bias):
    rows_f32 = token_rows.astype(jnp.float32)
    centered = rows_f32 - jnp.mean(rows_f32, axis=-1, keepdims=True)
    inv_std = lax.rsqrt(jnp.mean(centered * centered, axis=-1, keepdims=True) + LN_EPS)
    x_hat = centered * inv_std
    return x_hat, inv_std, (x_hat * norm_gain + norm_bias).astype(jnp.bfloat16)


def layer_norm_bwd(grad_norm, x_hat, inv_std, norm_gain):
    grad_hat = grad_norm * norm_gain
    centered_grad = grad_hat - jnp.mean(grad_hat, axis=-1, keepdims=True)
    return inv_std * (centered_grad - x_hat * jnp.mean(grad_hat * x_hat, axis=-1, keepdims=True))


def gelu_parts(pre_act):
    tanh_val = jnp.tanh(GELU_SCALE * (pre_act + GELU_COEF * pre_act * pre_act * pre_act))
    act_value = 0.5 * pre_act * (1.0 + tanh_val)
    act_slope = 0.5 * (1.0 + tanh_val) + 0.5 * pre_act * (1.0 - tanh_val * tanh_val) * GELU_SCALE * (1.0 + 3.0 * GELU_COEF * pre_act * pre_act)
    return act_value, act_slope


def dot_nn(a, b):
    return jnp.dot(a, b, preferred_element_type=jnp.float32)


def dot_nt(a, b):
    return lax.dot_general(a, b, (((1,), (1,)), ((), ())), preferred_element_type=jnp.float32)


def fold_rows(vals, op):
    rows, cols = vals.shape
    return op(vals.reshape(rows // 8, 8, cols), axis=0)


def attn_kernel(n_blk, dmid_ref, wo_ref, qt_ref, kt_ref, vt_ref, dqkv_ref, dwo_ref,
                k_s, v_s, dk_s, dv_s, dctx_s, ctx_s, st_s, pt_s, dpt_s, dst_s):
    row = n_blk - 1 - pl.program_id(0)
    head = pl.program_id(1)
    n_heads = pl.num_programs(1)
    hd = qt_ref.shape[1]
    scale = hd ** -0.5

    @pl.when(head == 0)
    def _():
        dctx_s[...] = dot_nt(wo_ref[...], dmid_ref[...]).astype(jnp.bfloat16).reshape(dctx_s.shape)

    @pl.when(pl.program_id(0) == 0)
    def _():
        for c in range(n_blk):
            cols = slice(c * QB, (c + 1) * QB)
            k_s[head, cols, :] = kt_ref[head, :, cols].T
            v_s[head, cols, :] = vt_ref[head, :, cols].T

    qt = qt_ref[head]
    dot_ = dctx_s[head]

    def body(n):
        first = n == n_blk
        mx = None
        for c in range(n):
            cols = slice(c * QB, (c + 1) * QB)
            st = dot_nn(k_s[head, cols, :], qt)
            if c == n - 1:
                kv_ids = lax.broadcasted_iota(jnp.int32, (QB, QB), 0)
                q_ids = lax.broadcasted_iota(jnp.int32, (QB, QB), 1)
                st = jnp.where(kv_ids <= q_ids, st, NEG)
            st_s[cols, :] = st
            part = fold_rows(st, jnp.max)
            mx = part if mx is None else jnp.maximum(mx, part)
        shift = jnp.max(mx, axis=0, keepdims=True) * (scale * LOG2E)
        tot = None
        for c in range(n):
            cols = slice(c * QB, (c + 1) * QB)
            ex = jnp.exp2(st_s[cols, :] * (scale * LOG2E) - shift)
            st_s[cols, :] = ex
            part = fold_rows(ex, jnp.sum)
            tot = part if tot is None else tot + part
        inv = 1.0 / jnp.sum(tot, axis=0, keepdims=True)
        dsum = None
        for c in range(n):
            cols = slice(c * QB, (c + 1) * QB)
            prob = st_s[cols, :] * inv
            st_s[cols, :] = prob
            pb = prob.astype(jnp.bfloat16)
            pt_s[cols, :] = pb
            dp = dot_nn(v_s[head, cols, :], dot_)
            dpt_s[cols, :] = dp
            part = fold_rows(dp * prob, jnp.sum)
            dsum = part if dsum is None else dsum + part
            dv = dot_nt(pb, dot_)
            dv_s[head, cols, :] = dv if first else dv_s[head, cols, :] + dv
        dsum = jnp.sum(dsum, axis=0, keepdims=True)
        ctx_s[head] = dot_nn(vt_ref[head, :, :n * QB], pt_s[:n * QB, :]).astype(jnp.bfloat16)
        for c in range(n):
            cols = slice(c * QB, (c + 1) * QB)
            ds = (st_s[cols, :] * (dpt_s[cols, :] - dsum) * scale).astype(jnp.bfloat16)
            dst_s[cols, :] = ds
            dk = dot_nt(ds, qt)
            dk_s[head, cols, :] = dk if first else dk_s[head, cols, :] + dk
        dqkv_ref[0, head] = dot_nn(kt_ref[head, :, :n * QB], dst_s[:n * QB, :]).astype(jnp.bfloat16)
        last = slice((n - 1) * QB, n * QB)
        dqkv_ref[1, head] = dk_s[head, last, :].T.astype(jnp.bfloat16)
        dqkv_ref[2, head] = dv_s[head, last, :].T.astype(jnp.bfloat16)

    for n in range(1, n_blk + 1):
        pl.when(row == n - 1)(functools.partial(body, n))

    @pl.when(head == n_heads - 1)
    def _():
        ctx = ctx_s[...].reshape(dwo_ref.shape[0], QB)
        term = dot_nn(ctx, dmid_ref[...])

        @pl.when(pl.program_id(0) == 0)
        def _():
            dwo_ref[...] = term

        @pl.when(pl.program_id(0) > 0)
        def _():
            dwo_ref[...] += term


def attention_bwd(dmid, wo, qt, kt, vt):
    n_tok, dm = dmid.shape
    n_heads, hd, _ = qt.shape
    n_blk = n_tok // QB
    full3 = pl.BlockSpec((n_heads, hd, n_tok), lambda i, h: (0, 0, 0), pipeline_mode=pl.Buffered(1))
    flops = 6 * 2 * n_heads * n_tok * n_tok * 256 // 2 + 8 * n_tok * dm * n_heads * hd
    return pl.pallas_call(
        functools.partial(attn_kernel, n_blk),
        grid=(n_blk, n_heads),
        out_shape=(jax.ShapeDtypeStruct((3, n_heads, hd, n_tok), jnp.bfloat16),
                   jax.ShapeDtypeStruct((n_heads * hd, dm), jnp.float32)),
        in_specs=[
            pl.BlockSpec((QB, dm), lambda i, h: (n_blk - 1 - i, 0)),
            pl.BlockSpec((n_heads * hd, dm), lambda i, h: (0, 0), pipeline_mode=pl.Buffered(1)),
            pl.BlockSpec((n_heads, hd, QB), lambda i, h: (0, 0, n_blk - 1 - i)),
            full3, full3,
        ],
        out_specs=(
            pl.BlockSpec((3, n_heads, hd, QB), lambda i, h: (0, 0, 0, n_blk - 1 - i)),
            pl.BlockSpec((n_heads * hd, dm), lambda i, h: (0, 0)),
        ),
        scratch_shapes=[
            pltpu.VMEM((n_heads, n_tok, hd), jnp.bfloat16),
            pltpu.VMEM((n_heads, n_tok, hd), jnp.bfloat16),
            pltpu.VMEM((n_heads, n_tok, hd), jnp.float32),
            pltpu.VMEM((n_heads, n_tok, hd), jnp.float32),
            pltpu.VMEM((n_heads, hd, QB), jnp.bfloat16),
            pltpu.VMEM((n_heads, hd, QB), jnp.bfloat16),
            pltpu.VMEM((n_tok, QB), jnp.float32),
            pltpu.VMEM((n_tok, QB), jnp.bfloat16),
            pltpu.VMEM((n_tok, QB), jnp.float32),
            pltpu.VMEM((n_tok, QB), jnp.bfloat16),
        ],
        compiler_params=pltpu.CompilerParams(dimension_semantics=("arbitrary", "arbitrary"),
                                             vmem_limit_bytes=56 * 1024 * 1024),
        cost_estimate=pl.CostEstimate(flops=flops, bytes_accessed=20_000_000, transcendentals=0),
        name="attn_bwd",
    )(dmid, wo, qt, kt, vt)


def solution(mesh):
    def local_backward(x_in, x_mid, d_out, q_saved, k_saved, v_saved, z_saved, ln1_gain, ln1_bias, ln2_gain, ln2_bias, w_qkv, w_proj, w_fc1, w_fc2):
        norm2_hat, norm2_rstd, h2_local = layer_norm_fwd(x_mid, ln2_gain, ln2_bias)
        h2_full = lax.all_gather(h2_local, 'tp', axis=1, tiled=True)
        dout_full = lax.all_gather(d_out, 'tp', axis=1, tiled=True)
        act_value, act_slope = gelu_parts(z_saved.astype(jnp.float32))
        grad_wfc2 = jnp.einsum('bsf,bsd->fd', act_value.astype(jnp.bfloat16), dout_full, preferred_element_type=jnp.float32)
        grad_pre = (jnp.einsum('bsd,fd->bsf', dout_full, w_fc2, preferred_element_type=jnp.float32) * act_slope).astype(jnp.bfloat16)
        grad_wfc1 = jnp.einsum('bsd,bsf->df', h2_full, grad_pre, preferred_element_type=jnp.float32)
        grad_bfc1 = jnp.sum(grad_pre, axis=(0, 1), dtype=jnp.float32)
        h2_partial = jnp.einsum('bsf,df->bsd', grad_pre, w_fc1, preferred_element_type=jnp.float32).astype(jnp.bfloat16)
        grad_h2 = lax.psum_scatter(h2_partial, 'tp', scatter_dimension=1, tiled=True).astype(jnp.float32)
        grad_mid = (d_out.astype(jnp.float32) + layer_norm_bwd(grad_h2, norm2_hat, norm2_rstd, ln2_gain)).astype(jnp.bfloat16)
        mid_full = lax.all_gather(grad_mid, 'tp', axis=1, tiled=True)
        norm1_hat, norm1_rstd, h1_local = layer_norm_fwd(x_in, ln1_gain, ln1_bias)
        h1_full = lax.all_gather(h1_local, 'tp', axis=1, tiled=True)
        n_tok, d_model = mid_full.shape[1:]
        qt, kt, vt = (t[0].transpose(1, 2, 0) for t in (q_saved, k_saved, v_saved))
        n_heads, head_dim = qt.shape[:2]
        dqkv, dwo = attention_bwd(mid_full[0], w_proj.reshape(-1, d_model), qt, kt, vt)
        grad_wproj = dwo.reshape(w_proj.shape)
        flat = dqkv.reshape(-1, n_tok)
        w_rows = w_qkv.transpose(0, 2, 3, 1).reshape(-1, d_model)
        grad_wqkv = dot_nn(flat, h1_full[0]).reshape(3, n_heads, head_dim, d_model).transpose(0, 3, 1, 2)
        grad_bqkv = jnp.sum(dqkv, axis=-1, dtype=jnp.float32)
        h1_partial = lax.dot_general(flat, w_rows, (((0,), (0,)), ((), ())), preferred_element_type=jnp.float32).astype(jnp.bfloat16)[None]
        grad_h1 = lax.psum_scatter(h1_partial, 'tp', scatter_dimension=1, tiled=True).astype(jnp.float32)
        grad_x = (grad_mid.astype(jnp.float32) + layer_norm_bwd(grad_h1, norm1_hat, norm1_rstd, ln1_gain)).astype(jnp.bfloat16)
        vec_partial = jnp.stack([
            jnp.sum(grad_h1 * norm1_hat, axis=(0, 1)),
            jnp.sum(grad_h1, axis=(0, 1)),
            jnp.sum(grad_h2 * norm2_hat, axis=(0, 1)),
            jnp.sum(grad_h2, axis=(0, 1)),
            jnp.sum(grad_mid, axis=(0, 1), dtype=jnp.float32),
            jnp.sum(d_out, axis=(0, 1), dtype=jnp.float32),
        ])
        grad_vecs = lax.psum(vec_partial, 'tp')
        return grad_x, grad_wqkv, grad_bqkv, grad_wproj, grad_wfc1, grad_bfc1, grad_wfc2, grad_vecs

    tok_spec = P('dp', 'tp', None)
    head_spec = P('dp', None, 'tp', None)
    in_specs = (tok_spec, tok_spec, tok_spec, head_spec, head_spec, head_spec, P('dp', None, 'tp'),
                P(None), P(None), P(None), P(None),
                P(None, None, 'tp', None), P('tp', None, None), P(None, 'tp'), P('tp', None))
    out_specs = (tok_spec, P('dp', None, 'tp', None), P('dp', 'tp', None), P(('dp', 'tp'), None, None),
                 P('dp', 'tp'), P(('dp', 'tp')), P(('dp', 'tp'), None), P('dp', None))
    return jax.shard_map(local_backward, mesh=mesh, in_specs=in_specs, out_specs=out_specs, check_vma=False)
```

```python
import functools

import jax
import jax.numpy as jnp
from jax import lax
from jax.experimental import pallas as pl
from jax.experimental.pallas import tpu as pltpu
from jax.sharding import PartitionSpec as P

LN_EPS = 1e-5
GELU_COEF = 0.044715
GELU_SCALE = 0.7978845608028654
LOG2E = 1.4426950408889634
NEG = -1e30
QB = 256
BF = jnp.bfloat16
F32 = jnp.float32
VMEM_CAP = 66_000_000

def layer_norm_fwd(token_rows, norm_gain, norm_bias):
    rows_f32 = token_rows.astype(jnp.float32)
    centered = rows_f32 - jnp.mean(rows_f32, axis=-1, keepdims=True)
    inv_std = lax.rsqrt(jnp.mean(centered * centered, axis=-1, keepdims=True) + LN_EPS)
    x_hat = centered * inv_std
    return x_hat, inv_std, (x_hat * norm_gain + norm_bias).astype(jnp.bfloat16)


def layer_norm_bwd(grad_norm, x_hat, inv_std, norm_gain):
    grad_hat = grad_norm * norm_gain
    centered_grad = grad_hat - jnp.mean(grad_hat, axis=-1, keepdims=True)
    return inv_std * (centered_grad - x_hat * jnp.mean(grad_hat * x_hat, axis=-1, keepdims=True))


def gelu_parts(pre_act):
    tanh_val = jnp.tanh(GELU_SCALE * (pre_act + GELU_COEF * pre_act * pre_act * pre_act))
    act_value = 0.5 * pre_act * (1.0 + tanh_val)
    act_slope = 0.5 * (1.0 + tanh_val) + 0.5 * pre_act * (1.0 - tanh_val * tanh_val) * GELU_SCALE * (1.0 + 3.0 * GELU_COEF * pre_act * pre_act)
    return act_value, act_slope


def dot_nn(a, b):
    return jnp.dot(a, b, preferred_element_type=jnp.float32)


def dot_nt(a, b):
    return lax.dot_general(a, b, (((1,), (1,)), ((), ())), preferred_element_type=jnp.float32)


def fold_rows(vals, op):
    rows, cols = vals.shape
    return op(vals.reshape(rows // 8, 8, cols), axis=0)


def attn_kernel(n_blk, tbl_ref, *refs):
    dmid_refs, refs = refs[:n_blk], refs[n_blk:]
    (wo_ref, qt_ref, kt_ref, vt_ref, dqkv_ref, dwo_ref,
     k_s, v_s, dk_s, dv_s, dctx_s, ctx_s, st_s, pt_s, dpt_s, dst_s, dmid_s) = refs
    row = n_blk - 1 - pl.program_id(0)
    head = pl.program_id(1)
    n_heads = pl.num_programs(1)
    hd = qt_ref.shape[1]
    scale = hd ** -0.5

    @pl.when(head == 0)
    def _():
        for r in range(n_blk):
            @pl.when(row == 2 * tbl_ref[r // 2] + r % 2)
            def _():
                dmid_s[...] = dmid_refs[r][...]
        dctx_s[...] = dot_nt(wo_ref[...], dmid_s[...]).astype(jnp.bfloat16).reshape(dctx_s.shape)

    @pl.when(pl.program_id(0) == 0)
    def _():
        for c in range(n_blk):
            cols = slice(c * QB, (c + 1) * QB)
            k_s[head, cols, :] = kt_ref[head, :, cols].T
            v_s[head, cols, :] = vt_ref[head, :, cols].T

    qt = qt_ref[head]
    dot_ = dctx_s[head]

    def body(n):
        first = n == n_blk
        mx = None
        for c in range(n):
            cols = slice(c * QB, (c + 1) * QB)
            st = dot_nn(k_s[head, cols, :], qt)
            if c == n - 1:
                kv_ids = lax.broadcasted_iota(jnp.int32, (QB, QB), 0)
                q_ids = lax.broadcasted_iota(jnp.int32, (QB, QB), 1)
                st = jnp.where(kv_ids <= q_ids, st, NEG)
            st_s[cols, :] = st
            part = fold_rows(st, jnp.max)
            mx = part if mx is None else jnp.maximum(mx, part)
        shift = jnp.max(mx, axis=0, keepdims=True) * (scale * LOG2E)
        tot = None
        for c in range(n):
            cols = slice(c * QB, (c + 1) * QB)
            ex = jnp.exp2(st_s[cols, :] * (scale * LOG2E) - shift)
            st_s[cols, :] = ex
            part = fold_rows(ex, jnp.sum)
            tot = part if tot is None else tot + part
        inv = 1.0 / jnp.sum(tot, axis=0, keepdims=True)
        dsum = None
        for c in range(n):
            cols = slice(c * QB, (c + 1) * QB)
            prob = st_s[cols, :] * inv
            st_s[cols, :] = prob
            pb = prob.astype(jnp.bfloat16)
            pt_s[cols, :] = pb
            dp = dot_nn(v_s[head, cols, :], dot_)
            dpt_s[cols, :] = dp
            part = fold_rows(dp * prob, jnp.sum)
            dsum = part if dsum is None else dsum + part
            dv = dot_nt(pb, dot_)
            dv_s[head, cols, :] = dv if first else dv_s[head, cols, :] + dv
        dsum = jnp.sum(dsum, axis=0, keepdims=True)
        ctx_s[head] = dot_nn(vt_ref[head, :, :n * QB], pt_s[:n * QB, :]).astype(jnp.bfloat16)
        for c in range(n):
            cols = slice(c * QB, (c + 1) * QB)
            ds = (st_s[cols, :] * (dpt_s[cols, :] - dsum) * scale).astype(jnp.bfloat16)
            dst_s[cols, :] = ds
            dk = dot_nt(ds, qt)
            dk_s[head, cols, :] = dk if first else dk_s[head, cols, :] + dk
        dqkv_ref[0, head] = dot_nn(kt_ref[head, :, :n * QB], dst_s[:n * QB, :]).astype(jnp.bfloat16)
        last = slice((n - 1) * QB, n * QB)
        dqkv_ref[1, head] = dk_s[head, last, :].T.astype(jnp.bfloat16)
        dqkv_ref[2, head] = dv_s[head, last, :].T.astype(jnp.bfloat16)

    for n in range(1, n_blk + 1):
        pl.when(row == n - 1)(functools.partial(body, n))

    @pl.when(head == n_heads - 1)
    def _():
        ctx = ctx_s[...].reshape(dwo_ref.shape[0], QB)
        term = dot_nn(ctx, dmid_s[...])

        @pl.when(pl.program_id(0) == 0)
        def _():
            dwo_ref[...] = term

        @pl.when(pl.program_id(0) > 0)
        def _():
            dwo_ref[...] += term


def attention_bwd(tbl, dmids, wo, qt, kt, vt):
    dm = wo.shape[1]
    n_heads, hd, n_tok = qt.shape
    n_blk = n_tok // QB
    full3 = pl.BlockSpec((n_heads, hd, n_tok), lambda i, h, t: (0, 0, 0), pipeline_mode=pl.Buffered(1))
    blk = pl.BlockSpec((QB, dm), lambda i, h, t: (0, 0), pipeline_mode=pl.Buffered(1))
    flops = 6 * 2 * n_heads * n_tok * n_tok * 256 // 2 + 8 * n_tok * dm * n_heads * hd
    return pl.pallas_call(
        functools.partial(attn_kernel, n_blk),
        grid_spec=pltpu.PrefetchScalarGridSpec(
            num_scalar_prefetch=1,
            grid=(n_blk, n_heads),
            in_specs=[blk] * n_blk + [
                pl.BlockSpec((n_heads * hd, dm), lambda i, h, t: (0, 0), pipeline_mode=pl.Buffered(1)),
                pl.BlockSpec((n_heads, hd, QB), lambda i, h, t: (0, 0, n_blk - 1 - i)),
                full3, full3,
            ],
            out_specs=(
                pl.BlockSpec((3, n_heads, hd, QB), lambda i, h, t: (0, 0, 0, n_blk - 1 - i)),
                pl.BlockSpec((n_heads * hd, dm), lambda i, h, t: (0, 0)),
            ),
            scratch_shapes=[
                pltpu.VMEM((n_heads, n_tok, hd), BF),
                pltpu.VMEM((n_heads, n_tok, hd), BF),
                pltpu.VMEM((n_heads, n_tok, hd), F32),
                pltpu.VMEM((n_heads, n_tok, hd), F32),
                pltpu.VMEM((n_heads, hd, QB), BF),
                pltpu.VMEM((n_heads, hd, QB), BF),
                pltpu.VMEM((n_tok, QB), F32),
                pltpu.VMEM((n_tok, QB), BF),
                pltpu.VMEM((n_tok, QB), F32),
                pltpu.VMEM((n_tok, QB), BF),
                pltpu.VMEM((QB, dm), BF),
            ]),
        out_shape=(jax.ShapeDtypeStruct((3, n_heads, hd, n_tok), BF),
                   jax.ShapeDtypeStruct((n_heads * hd, dm), F32)),
        compiler_params=pltpu.CompilerParams(dimension_semantics=("arbitrary", "arbitrary"),
                                             vmem_limit_bytes=VMEM_CAP),
        cost_estimate=pl.CostEstimate(flops=flops * 2, bytes_accessed=20_000_000, transcendentals=0),
        name="attn_bwd",
    )(tbl, *dmids, wo, qt, kt, vt)


def mlp_kernel(tbl_ref, dya_ref, dyb_ref, za_ref, zb_ref, w2_ref, w1_ref,
               dza_ref, dzb_ref, ua_ref, ub_ref, pa_ref, pb_ref, db_ref, dy_s, dz_s):
    half = QB
    n_ff, dm = w2_ref.shape
    dy_s[:half, :] = dya_ref[...]
    dy_s[half:, :] = dyb_ref[...]

    @pl.when(pl.program_id(0) == 0)
    def _():
        db_ref[...] = jnp.zeros_like(db_ref)

    for j in range(n_ff // 256):
        cols = slice(j * 256, (j + 1) * 256)
        acc = dot_nt(dy_s[...], w2_ref[cols, :])
        part = None
        for z_ref, dz_ref, u_ref, lo in ((za_ref, dza_ref, ua_ref, 0), (zb_ref, dzb_ref, ub_ref, half)):
            act, slope = gelu_parts(z_ref[:, cols].astype(F32))
            u_ref[:, cols] = act.astype(BF)
            dz = (acc[lo:lo + half, :] * slope).astype(BF)
            dz_ref[:, cols] = dz
            dz_s[lo:lo + half, cols] = dz
            fold = fold_rows(dz.astype(F32), jnp.sum)
            part = fold if part is None else part + fold
        db_ref[:, cols] += part
    for j in range(dm // 256):
        cols = slice(j * 256, (j + 1) * 256)
        acc = dot_nt(dz_s[...], w1_ref[cols, :]).astype(BF)
        pa_ref[:, cols] = acc[:half, :]
        pb_ref[:, cols] = acc[half:, :]


def mlp_bwd(blks, dya, dyb, z, w2, w1):
    rows, dm = dya.shape
    n_ff = w2.shape[0]
    row = pl.BlockSpec((QB, dm), lambda g, t: (g, 0))
    wide = pl.BlockSpec((QB, n_ff), lambda g, t: (g, 0))
    out = jax.ShapeDtypeStruct((rows, n_ff), BF)
    part = jax.ShapeDtypeStruct((rows, dm), BF)
    return pl.pallas_call(
        mlp_kernel,
        grid_spec=pltpu.PrefetchScalarGridSpec(
            num_scalar_prefetch=1,
            grid=(rows // QB,),
            in_specs=[row, row,
                      pl.BlockSpec((QB, n_ff), lambda g, t: (t[0] + g, 0)),
                      pl.BlockSpec((QB, n_ff), lambda g, t: (t[1] + g, 0)),
                      pl.BlockSpec((n_ff, dm), lambda g, t: (0, 0), pipeline_mode=pl.Buffered(1)),
                      pl.BlockSpec((dm, n_ff), lambda g, t: (0, 0), pipeline_mode=pl.Buffered(1))],
            out_specs=(wide, wide, wide, wide, row, row, pl.BlockSpec((8, n_ff), lambda g, t: (0, 0))),
            scratch_shapes=[pltpu.VMEM((2 * QB, dm), BF), pltpu.VMEM((2 * QB, n_ff), BF)]),
        out_shape=(out, out, out, out, part, part, jax.ShapeDtypeStruct((8, n_ff), F32)),
        compiler_params=pltpu.CompilerParams(dimension_semantics=("arbitrary",), vmem_limit_bytes=VMEM_CAP),
        cost_estimate=pl.CostEstimate(flops=2 * 4 * 2 * rows * dm * n_ff, bytes_accessed=20_000_000, transcendentals=0),
        name="mlp_bwd",
    )(blks, dya, dyb, z, z, w2, w1)


def dw_kernel(n_a, cuts, *refs):
    a_refs, b_refs, (o_ref, tok_ref, at_s) = refs[:n_a], refs[n_a:-3], refs[-3:]
    tok_ref[...] = jnp.zeros_like(tok_ref)
    lo = 0
    for a_ref in a_refs:
        rows = a_ref.shape[0]
        for r in range(0, rows, 256):
            at_s[:, lo:lo + 256] = a_ref[r:r + 256, :].T
            lo += 256
    for j in range(o_ref.shape[1] // 256):
        cols = slice(j * 256, (j + 1) * 256)
        acc = None
        lo = 0
        for b_ref in b_refs:
            rows = b_ref.shape[0]
            term = dot_nn(at_s[:, lo:lo + rows], b_ref[:, cols])
            acc = term if acc is None else acc + term
            lo += rows
        o_ref[:, cols] = acc


def weight_grad(a_list, b_list):
    n_a = a_list[0].shape[1]
    n_b = b_list[0].shape[1]
    n_tok = sum(a.shape[0] for a in a_list)
    return pl.pallas_call(
        functools.partial(dw_kernel, len(a_list), None),
        grid=(n_a // 256,),
        in_specs=[pl.BlockSpec((a.shape[0], 256), lambda i: (0, i)) for a in a_list]
        + [pl.BlockSpec(b.shape, lambda i: (0, 0), pipeline_mode=pl.Buffered(1)) for b in b_list],
        out_specs=(pl.BlockSpec((256, n_b), lambda i: (i, 0)), pl.BlockSpec((8, 128), lambda i: (0, 0))),
        scratch_shapes=[pltpu.VMEM((256, n_tok), BF)],
        out_shape=(jax.ShapeDtypeStruct((n_a, n_b), F32), jax.ShapeDtypeStruct((8, 128), F32)),
        compiler_params=pltpu.CompilerParams(dimension_semantics=("arbitrary",), vmem_limit_bytes=48 * 1024 * 1024),
        cost_estimate=pl.CostEstimate(flops=2 * 2 * n_tok * n_a * n_b, bytes_accessed=20_000_000, transcendentals=0),
        name="weight_grad",
    )(*a_list, *b_list)


def dwqkv_kernel(tbl_ref, *refs):
    a_refs, b_refs, o_ref, tok_ref = refs[:4], refs[4:8], refs[8], refs[9]
    tok_ref[...] = jnp.zeros_like(tok_ref)
    for j in range(o_ref.shape[1] // 256):
        cols = slice(j * 256, (j + 1) * 256)
        acc = None
        for a_ref, b_ref in zip(a_refs, b_refs):
            term = dot_nn(a_ref[...], b_ref[:, cols])
            acc = term if acc is None else acc + term
        o_ref[:, cols] = acc


def dwqkv_grad(tbl, flat, h_list):
    n_out, n_tok = flat.shape
    dm = h_list[0].shape[1]
    rows = h_list[0].shape[0]
    tile = 384

    def spec(r):
        return pl.BlockSpec((tile, rows), lambda i, t: (i, t[r]))

    return pl.pallas_call(
        dwqkv_kernel,
        grid_spec=pltpu.PrefetchScalarGridSpec(
            num_scalar_prefetch=1,
            grid=(n_out // tile,),
            in_specs=[spec(r) for r in range(4)]
            + [pl.BlockSpec(h.shape, lambda i, t: (0, 0), pipeline_mode=pl.Buffered(1)) for h in h_list],
            out_specs=(pl.BlockSpec((tile, dm), lambda i, t: (i, 0)), pl.BlockSpec((8, 128), lambda i, t: (0, 0)))),
        out_shape=(jax.ShapeDtypeStruct((n_out, dm), F32), jax.ShapeDtypeStruct((8, 128), F32)),
        compiler_params=pltpu.CompilerParams(dimension_semantics=("arbitrary",), vmem_limit_bytes=48 * 1024 * 1024),
        cost_estimate=pl.CostEstimate(flops=2 * 2 * n_tok * n_out * dm, bytes_accessed=20_000_000, transcendentals=0),
        name="dwqkv",
    )(tbl, flat, flat, flat, flat, *h_list)


def dh1_kernel(tbl_ref, fa_ref, fb_ref, w_ref, pa_ref, pb_ref, ft_s):
    ft_s[:QB, :] = fa_ref[...].T
    ft_s[QB:, :] = fb_ref[...].T
    for j in range(w_ref.shape[1] // 256):
        cols = slice(j * 256, (j + 1) * 256)
        acc = dot_nn(ft_s[...], w_ref[:, cols]).astype(BF)
        pa_ref[:, cols] = acc[:QB, :]
        pb_ref[:, cols] = acc[QB:, :]


def dh1_part(blks, flat, w_rows, rows):
    n_out, dm = w_rows.shape
    row = pl.BlockSpec((QB, dm), lambda g, t: (g, 0))
    part = jax.ShapeDtypeStruct((rows, dm), BF)
    return pl.pallas_call(
        dh1_kernel,
        grid_spec=pltpu.PrefetchScalarGridSpec(
            num_scalar_prefetch=1,
            grid=(rows // QB,),
            in_specs=[pl.BlockSpec((n_out, QB), lambda g, t: (0, t[0] + g)),
                      pl.BlockSpec((n_out, QB), lambda g, t: (0, t[1] + g)),
                      pl.BlockSpec((n_out, dm), lambda g, t: (0, 0), pipeline_mode=pl.Buffered(1))],
            out_specs=(row, row),
            scratch_shapes=[pltpu.VMEM((2 * QB, n_out), BF)]),
        out_shape=(part, part),
        compiler_params=pltpu.CompilerParams(dimension_semantics=("arbitrary",), vmem_limit_bytes=48 * 1024 * 1024),
        cost_estimate=pl.CostEstimate(flops=2 * 2 * 2 * rows * dm * n_out, bytes_accessed=8_000_000, transcendentals=0),
        name="dh1_part",
    )(blks, flat, flat, w_rows)


ACROSS = [(0, 2), (1, 3), (2, 0), (3, 1)]
BESIDE = [(0, 1), (1, 0), (2, 3), (3, 2)]


def across(a):
    return lax.ppermute(a, 'tp', ACROSS)


def beside(a):
    return lax.ppermute(a, 'tp', BESIDE)


def after(a, *deps):
    return lax.optimization_barrier((a, *deps))[0]


def wide_add(a, b):
    return a.astype(F32) + b.astype(F32)


def solution(mesh):
    def local_backward(x_in, x_mid, d_out, q_saved, k_saved, v_saved, z_saved, ln1_gain, ln1_bias, ln2_gain, ln2_bias, w_qkv, w_proj, w_fc1, w_fc2):
        x0, x1, dy, z = x_in[0], x_mid[0], d_out[0], z_saved[0]
        d_model = dy.shape[1]
        me = lax.axis_index('tp').astype(jnp.int32)
        tbl = jnp.bitwise_xor(me, jnp.arange(4, dtype=jnp.int32))
        halves = (slice(0, QB), slice(QB, 2 * QB))

        xo = [across(dy[h]) for h in halves]
        sib = beside(dy)
        hat2, rstd2, h2 = layer_norm_fwd(x1, ln2_gain, ln2_bias)
        hat1, rstd1, h1 = layer_norm_fwd(x0, ln1_gain, ln1_bias)

        dz_o, dz_s, u_o, u_s, p_o, p_s, db_0 = mlp_bwd(2 * tbl[:2], dy, sib, z, w_fc2, w_fc1)
        r_o = beside(p_s)
        xo = [after(t, db_0) for t in xo]
        xs = [beside(t) for t in xo]
        far = []
        prev = db_0
        for i in range(2):
            far.append(mlp_bwd(after(2 * tbl[2:] + i, prev), xo[i], xs[i], z, w_fc2, w_fc1))
            prev = far[i][6]
        rx = [across(wide_add(f[4], beside(f[5])).astype(BF)) for f in far]
        grad_wfc2, tok_w2 = weight_grad([u_o, u_s] + [f[i] for f in far for i in (2, 3)], [dy, sib, xo[0], xs[0], xo[1], xs[1]])
        rx = [after(t, tok_w2) for t in rx]
        dh2 = [wide_add(p_o[h], r_o[h]) + rx[i].astype(F32) for i, h in enumerate(halves)]
        mid = [(dy[h].astype(F32) + layer_norm_bwd(dh2[i], hat2[h], rstd2[h], ln2_gain)).astype(BF) for i, h in enumerate(halves)]
        mid_xo = [across(m) for m in mid]
        mid_s = [beside(m) for m in mid]
        mid_xs = [beside(m) for m in mid_xo]
        h2, h1 = after(h2, mid[1]), after(h1, mid[1])
        h1_xo = across(h1)
        h2_xo = across(h2)
        h1_s, h2_s = beside(h1), beside(h2)
        h1_xs, h2_xs = beside(h1_xo), beside(h2_xo)

        grad_bfc1 = jnp.sum(db_0 + far[0][6] + far[1][6], axis=0)

        qt, kt, vt = (t[0].transpose(1, 2, 0) for t in (q_saved, k_saved, v_saved))
        n_heads, head_dim, n_tok = qt.shape
        dqkv, dwo = attention_bwd(tbl, mid + mid_s + mid_xo + mid_xs, w_proj.reshape(-1, d_model), qt, kt, vt)
        grad_wproj = dwo.reshape(w_proj.shape)
        flat = dqkv.reshape(-1, n_tok)
        w_rows = w_qkv.transpose(0, 2, 3, 1).reshape(-1, d_model)
        g_far = [dh1_part(2 * tbl[2:] + i, flat, w_rows, QB) for i in range(2)]
        g_sum = [wide_add(a, beside(b)).astype(BF) for a, b in g_far]
        gx = [across(t) for t in g_sum]
        g_o, g_s = dh1_part(after(2 * tbl[:2], *g_sum), flat, w_rows, 2 * QB)
        g_r = beside(g_s)
        d_rows, tok_qkv = dwqkv_grad(tbl, flat, [h1, h1_s, h1_xo, h1_xs])
        grad_wqkv = d_rows.reshape(3, n_heads, head_dim, d_model).transpose(0, 3, 1, 2)
        grad_bqkv = jnp.sum(dqkv, axis=-1, dtype=F32)
        grad_wfc1, tok_w1 = weight_grad([h2, h2_s, h2_xo, h2_xs], [dz_o, dz_s, far[0][0], far[1][0], far[0][1], far[1][1]])
        gx = [after(t, tok_qkv, tok_w1) for t in gx]
        dh1 = [wide_add(g_o[h], g_r[h]) + gx[i].astype(F32) for i, h in enumerate(halves)]
        grad_x = jnp.concatenate([
            (mid[i].astype(F32) + layer_norm_bwd(dh1[i], hat1[h], rstd1[h], ln1_gain)).astype(BF) for i, h in enumerate(halves)])[None]

        def group_sum(v):
            v = v + beside(v)
            return v + across(v)

        def tok_sum(parts):
            return sum(jnp.sum(p.astype(F32), axis=0) for p in parts)

        late = group_sum(jnp.stack([
            tok_sum([dh1[i] * hat1[h] for i, h in enumerate(halves)]),
            tok_sum(dh1),
        ]))
        early = group_sum(jnp.stack([
            tok_sum([dh2[i] * hat2[h] for i, h in enumerate(halves)]),
            tok_sum(dh2),
            tok_sum(mid),
            tok_sum([dy]),
        ]))
        return grad_x, grad_wqkv, grad_bqkv, grad_wproj, grad_wfc1, grad_bfc1, grad_wfc2, jnp.concatenate([late, early])

    tok_spec = P('dp', 'tp', None)
    head_spec = P('dp', None, 'tp', None)
    in_specs = (tok_spec, tok_spec, tok_spec, head_spec, head_spec, head_spec, P('dp', None, 'tp'),
                P(None), P(None), P(None), P(None),
                P(None, None, 'tp', None), P('tp', None, None), P(None, 'tp'), P('tp', None))
    out_specs = (tok_spec, P('dp', None, 'tp', None), P('dp', 'tp', None), P(('dp', 'tp'), None, None),
                 P('dp', 'tp'), P(('dp', 'tp')), P(('dp', 'tp'), None), P('dp', None))
    return jax.shard_map(local_backward, mesh=mesh, in_specs=in_specs, out_specs=out_specs, check_vma=False)
```
